32 devices in a mesh: af: 4 (over y, x), sa: 8 (over z, core).
Axes of the slice: x: 2, y: 2, z: 4, core: 2. Of those that a mesh axis runs over, the one named last changes fastest.
Arguments:
- data_real: bfloat16 [64, 512, 512], P('af', 'sa'), may hold values from -0.5 to 0.5
- data_imaginary: bfloat16 [64, 512, 512], P('af', 'sa'), may hold values from -0.5 to 0.5
- wavelet_real: float32 [64], P('af'), may hold values from -2.5 to 2.5
- wavelet_imaginary: float32 [64], P('af'), may hold values from -2.5 to 2.5
- primaries_real: float32 [64, 512, 512], P('af', 'sa'), may hold values from -3 to 3
- primaries_imaginary: float32 [64, 512, 512], P('af', 'sa'), may hold values from -3 to 3
Outputs:
- updated_real: float32 [64, 512, 512], P('af', 'sa')
- updated_imaginary: float32 [64, 512, 512], P('af', 'sa')
- misfit: float32 [2], replicated
The draws below stay inside these ranges and needn't reach their ends.
All inputs are finite; a program needn't handle non-finite values.
Results may differ from the reference program's by a relative error of at most 0.0018.
Values may be sent and summed in bfloat16 or wider, within the bound.
No kernel may reach another device: no remote copies, remote signals or barrier semaphores. Data moves between devices by JAX's collectives and lax.ppermute only.
A program may use at most 128 MiB of HBM per device.

```python
import jax
import jax.numpy as jnp
from jax import lax

N = 512
F = 64
ITERS = 2


def levels(own_key, dims, cuts, low, top_value):
    gain, own = 1.0, jax.random.fold_in(own_key, 6)
    for axis_at, parts in cuts:
        steps = jnp.exp(jax.random.uniform(jax.random.fold_in(own, axis_at), (parts,), jnp.float32, low / len(cuts), top_value / len(cuts)))
        gain = gain * jnp.repeat(steps, dims[axis_at] // parts).reshape([-1 if axis == axis_at else 1 for axis in range(len(dims))])
    return gain


def scatter_about(rng, shape, deviation, most, pieces=(), kind=jnp.bfloat16):
    gain = levels(rng, shape, pieces, -0.22, 0.18) if pieces else 1.0
    result = jax.random.normal(rng, shape, jnp.float32) * deviation * gain
    return jnp.minimum(jnp.maximum(result, -most), most).astype(kind)


def setup_inputs(seed: int = 0) -> dict:
    streams_of = jax.random.split(jax.random.key(seed), 7)
    data_real = scatter_about(streams_of[0], (F, N, N), (N // 4) ** -0.5, 0.5, ((0, 4), (1, 8)))
    data_imaginary = scatter_about(streams_of[1], (F, N, N), (N // 4) ** -0.5, 0.5, ((0, 4), (1, 8)))
    wavelet_real = scatter_about(streams_of[2], (F,), 0.7, 2.5, ((0, 4),), jnp.float32)
    wavelet_imaginary = scatter_about(streams_of[3], (F,), 0.7, 2.5, ((0, 4),), jnp.float32)
    primaries_real = scatter_about(streams_of[4], (F, N, N), 0.5, 3.0, ((0, 4), (1, 8)), jnp.float32)
    primaries_imaginary = scatter_about(streams_of[5], (F, N, N), 0.5, 3.0, ((0, 4), (1, 8)), jnp.float32)
    return dict(data_real=data_real, data_imaginary=data_imaginary, wavelet_real=wavelet_real, wavelet_imaginary=wavelet_imaginary, primaries_real=primaries_real, primaries_imaginary=primaries_imaginary)


STEP_LENGTH = 0.02
THRESHOLD = 0.25


def forward_product(left, right):
    return jnp.einsum("frk,fkc->frc", left, right, precision=lax.Precision.HIGHEST)


def adjoint_product(left, right):
    return jnp.einsum("frk,fjk->frj", left, right, precision=lax.Precision.HIGHEST)


def rounded(values):
    return lax.optimization_barrier(values.astype(jnp.bfloat16)).astype(jnp.float32)


def reference(data_real, data_imaginary, wavelet_real, wavelet_imaginary, primaries_real, primaries_imaginary):
    slab_real = data_real.astype(jnp.float32)
    slab_imaginary = data_imaginary.astype(jnp.float32)
    wave_real = wavelet_real[:, None, None]
    wave_imaginary = wavelet_imaginary[:, None, None]
    current_real = primaries_real
    current_imaginary = primaries_imaginary
    misfits = []
    for iteration in range(ITERS):
        rounded_real = rounded(current_real)
        rounded_imaginary = rounded(current_imaginary)
        forward_real = forward_product(rounded_real, slab_real) - forward_product(rounded_imaginary, slab_imaginary)
        forward_imaginary = forward_product(rounded_real, slab_imaginary) + forward_product(rounded_imaginary, slab_real)
        error_real = slab_real + forward_real - (wave_real * current_real - wave_imaginary * current_imaginary)
        error_imaginary = slab_imaginary + forward_imaginary - (wave_real * current_imaginary + wave_imaginary * current_real)
        total = jnp.sum(error_real * error_real) + jnp.sum(error_imaginary * error_imaginary)
        misfits.append(total / (F * N * N))
        eb_real = rounded(error_real)
        eb_imaginary = rounded(error_imaginary)
        back_real = adjoint_product(eb_real, slab_real) + adjoint_product(eb_imaginary, slab_imaginary)
        back_imaginary = adjoint_product(eb_imaginary, slab_real) - adjoint_product(eb_real, slab_imaginary)
        gradient_real = wave_real * error_real + wave_imaginary * error_imaginary - back_real
        gradient_imaginary = wave_real * error_imaginary - wave_imaginary * error_real - back_imaginary
        stepped_real = current_real + STEP_LENGTH * gradient_real
        stepped_imaginary = current_imaginary + STEP_LENGTH * gradient_imaginary
        in_time = jnp.fft.ifft(stepped_real + 1j * stepped_imaginary, axis=0, norm="ortho")
        time_real = jnp.real(in_time)
        time_imaginary = jnp.imag(in_time)
        shrunk_real = time_real - jnp.clip(time_real, -THRESHOLD, THRESHOLD)
        shrunk_imaginary = time_imaginary - jnp.clip(time_imaginary, -THRESHOLD, THRESHOLD)
        in_frequency = jnp.fft.fft(shrunk_real + 1j * shrunk_imaginary, axis=0, norm="ortho")
        current_real = jnp.real(in_frequency).astype(jnp.float32)
        current_imaginary = jnp.imag(in_frequency).astype(jnp.float32)
    return current_real, current_imaginary, jnp.stack(misfits).astype(jnp.float32)
```

```python
import math
from functools import partial

import jax
import jax.numpy as jnp
from jax import lax
from jax.experimental import pallas as pl
from jax.experimental.pallas import tpu as pltpu
from jax.sharding import PartitionSpec as P

ITERS = 2
STEP_LENGTH = 0.02
THRESHOLD = 0.25
CHUNKS = 4
TOP = 15.0
TINY = 1e-30
RADIX = 8
HALF = math.sqrt(0.5)


def add(a, b):
    return (a[0] + b[0], a[1] + b[1])


def sub(a, b):
    return (a[0] - b[0], a[1] - b[1])


def turn(a, sign):
    return (-a[1], a[0]) if sign > 0 else (a[1], -a[0])


def dft4(x, sign):
    a, b = add(x[0], x[2]), sub(x[0], x[2])
    c, d = add(x[1], x[3]), turn(sub(x[1], x[3]), sign)
    return [add(a, c), add(b, d), sub(a, c), sub(b, d)]


def dft8(x, sign):
    even, odd = dft4(x[0::2], sign), dft4(x[1::2], sign)
    r, i = odd[1]
    w1 = (HALF * (r - i), HALF * (i + r)) if sign > 0 else (HALF * (r + i), HALF * (i - r))
    w2 = turn(odd[2], sign)
    r, i = odd[3]
    w3 = (HALF * (-r - i), HALF * (r - i)) if sign > 0 else (HALF * (i - r), HALF * (-i - r))
    odd = [odd[0], w1, w2, w3]
    return [add(even[k], odd[k]) for k in range(4)] + [sub(even[k], odd[k]) for k in range(4)]


def twiddle(a, k, total, sign):
    if k % total == 0:
        return a
    c = math.cos(2.0 * math.pi * k / total)
    s = sign * math.sin(2.0 * math.pi * k / total)
    return (a[0] * c - a[1] * s, a[0] * s + a[1] * c)


def exponent(largest):
    return jnp.ceil(jnp.log2(jnp.maximum(largest, TINY))) + 1.0


def shrink(values):
    return values - jnp.clip(values, -THRESHOLD, THRESHOLD)


def product_kernel(*refs, packed, base, parts, stacked_rows):
    if packed:
        wr, wi, g_real, g_imag, g_exp, own_r, own_i, whole, z_out, sum_out = refs
        scale = jnp.exp2(g_exp[:, 0] - TOP)
        now_r = jnp.concatenate([g_real[d, 0] * scale[d] for d in range(parts)], axis=1)
        now_i = jnp.concatenate([g_imag[d, 0] * scale[d] for d in range(parts)], axis=1)
    else:
        wr, wi, g_real, g_imag, own_r, own_i, whole, z_out, sum_out = refs
        now_r = g_real[0]
        now_i = g_imag[0]
    f = base + pl.program_id(0)
    qr, qi = wr[f], wi[f]
    rows, n = now_r.shape
    if stacked_rows:
        p_r = whole[:, 0, 0].reshape(n, n)
        p_i = whole[:, 1, 0].reshape(n, n)
    else:
        p_r = whole[0, 0]
        p_i = whole[1, 0]
    left = jnp.concatenate([now_r, now_i], axis=0).astype(jnp.bfloat16)
    with_r = jnp.dot(left, p_r, preferred_element_type=jnp.float32)
    with_i = jnp.dot(left, p_i, preferred_element_type=jnp.float32)
    e_r = own_r[0].astype(jnp.float32) + (with_r[:rows] - with_i[rows:]) - (qr * now_r - qi * now_i)
    e_i = own_i[0].astype(jnp.float32) + (with_i[:rows] + with_r[rows:]) - (qr * now_i + qi * now_r)
    wide = n // parts
    squares = (e_r * e_r + e_i * e_i).reshape(rows // 8, 8, n).sum(axis=0)
    total = squares[:, :wide]
    for d in range(1, parts):
        total = total + squares[:, d * wide : (d + 1) * wide]
    sum_out[0] = total
    eb = jnp.concatenate([e_r, e_i], axis=0).astype(jnp.bfloat16)
    dims = (((1,), (1,)), ((), ()))
    back_r = lax.dot_general(eb, p_r, dims, preferred_element_type=jnp.float32)
    back_i = lax.dot_general(eb, p_i, dims, preferred_element_type=jnp.float32)
    h_r = qr * e_r + qi * e_i - (back_r[:rows] + back_i[rows:])
    h_i = qr * e_i - qi * e_r - (back_r[rows:] - back_i[:rows])
    z_r = now_r + STEP_LENGTH * h_r
    z_i = now_i + STEP_LENGTH * h_i
    blocks = rows // 8
    cut_r = [z_r[:, d * wide : (d + 1) * wide].reshape(blocks, 8, wide) for d in range(parts)]
    cut_i = [z_i[:, d * wide : (d + 1) * wide].reshape(blocks, 8, wide) for d in range(parts)]
    largest = jnp.maximum(jnp.abs(cut_r[0]), jnp.abs(cut_i[0]))
    for d in range(1, parts):
        largest = jnp.maximum(largest, jnp.maximum(jnp.abs(cut_r[d]), jnp.abs(cut_i[d])))
    power = exponent(largest.max(axis=0))
    factor = jnp.exp2(TOP - power)
    for d in range(parts):
        z_out[d, 0, :blocks] = cut_r[d] * factor[None]
        z_out[d, 0, blocks : 2 * blocks] = cut_i[d] * factor[None]
        z_out[d, 0, 2 * blocks] = power


def product(chunk, wave_r, wave_i, current, data_r, data_i, whole, parts):
    packed = not isinstance(current, tuple)
    count, rows, n = data_r.shape
    span = count // CHUNKS
    base = chunk * span
    wide = n // parts
    blocks = rows // 8
    stacked_rows = whole.ndim == 5
    smem = pl.BlockSpec(memory_space=pltpu.SMEM)
    own = pl.BlockSpec((1, rows, n), lambda f: (base + f, 0, 0))
    if packed:
        ins = [current, current, current]
        cur = [
            pl.BlockSpec((parts, 1, rows, wide), lambda f: (0, base + f, 0, 0)),
            pl.BlockSpec((parts, 1, rows, wide), lambda f: (0, count + base + f, 0, 0)),
            pl.BlockSpec((parts, 1, rows, wide), lambda f: (0, 2 * count, 0, 0)),
        ]
    else:
        ins = list(current)
        cur = [own, own]
    if stacked_rows:
        far = pl.BlockSpec((whole.shape[0], 2, 1, rows, n), lambda f: (0, 0, f, 0, 0))
    else:
        far = pl.BlockSpec((2, 1, n, n), lambda f: (0, f, 0, 0))
    kernel = partial(
        product_kernel, packed=packed, base=base, parts=parts, stacked_rows=stacked_rows
    )
    return pl.pallas_call(
        kernel,
        grid=(span,),
        in_specs=[smem, smem] + cur + [own, own, far],
        out_specs=[
            pl.BlockSpec((parts, 1, 2 * blocks + 1, 8, wide), lambda f: (0, f, 0, 0, 0)),
            pl.BlockSpec((1, 8, wide), lambda f: (f, 0, 0)),
        ],
        out_shape=[
            jax.ShapeDtypeStruct((parts, span, 2 * blocks + 1, 8, wide), jnp.float32),
            jax.ShapeDtypeStruct((span, 8, wide), jnp.float32),
        ],
        cost_estimate=pl.CostEstimate(
            flops=span * 16 * rows * n * n, bytes_accessed=span * 6 * n * n, transcendentals=0
        ),
        name=f"product_{chunk}_{int(packed)}",
    )(wave_r, wave_i, *ins, data_r, data_i, whole)


def transform_kernel(*refs, parts, count, span, group):
    ins, out, buf_r, buf_i = refs[:-3], refs[-3], refs[-2], refs[-1]
    total = parts * count
    norm = 1.0 / math.sqrt(total)

    def one(b, carry):
        def load(f):
            src, rest = divmod(f, count)
            chunk, j = divmod(rest, span)
            re, im, ex = ins[3 * chunk : 3 * chunk + 3]
            scale = jnp.exp2(ex[src, j, 0] - TOP) * norm
            return (re[src, j, b] * scale, im[src, j, b] * scale)

        for f0 in range(RADIX):
            got = dft8([load(RADIX * f1 + f0) for f1 in range(RADIX)], 1)
            for t1 in range(RADIX):
                v = twiddle(got[t1], f0 * t1, total, 1)
                buf_r[f0, t1], buf_i[f0, t1] = v
        largest = None
        for t1 in range(RADIX):
            z = dft8([(buf_r[f0, t1], buf_i[f0, t1]) for f0 in range(RADIX)], 1)
            x = [(shrink(r), shrink(i)) for r, i in z]
            for r, i in x:
                m = jnp.maximum(jnp.abs(r), jnp.abs(i))
                largest = m if largest is None else jnp.maximum(largest, m)
            got = dft8(x, -1)
            for f0 in range(RADIX):
                v = twiddle(got[f0], f0 * t1, total, -1)
                buf_r[f0, t1], buf_i[f0, t1] = v
        power = exponent(largest * (1.5 * math.sqrt(total)))
        factor = jnp.exp2(TOP - power) * norm
        at = pl.ds(pl.multiple_of(b * 8, 8), 8)
        for f0 in range(RADIX):
            got = dft8([(buf_r[f0, t1], buf_i[f0, t1]) for t1 in range(RADIX)], -1)
            for f1 in range(RADIX):
                dst, j = divmod(RADIX * f1 + f0, count)
                out[dst, j, at] = got[f1][0] * factor
                out[dst, count + j, at] = got[f1][1] * factor
        for dst in range(parts):
            out[dst, 2 * count, at] = power
        return carry

    lax.fori_loop(0, group, one, 0)


def transform(pieces, rows):
    parts, span, _, _, wide = pieces[0].shape
    count = span * CHUNKS
    blocks = rows // 8
    group = 2 if blocks % 2 == 0 else 1
    steps = blocks // group
    specs, ins = [], []
    for piece in pieces:
        ins += [piece] * 3
        specs += [
            pl.BlockSpec((parts, span, group, 8, wide), lambda g: (0, 0, g, 0, 0)),
            pl.BlockSpec((parts, span, group, 8, wide), lambda g: (0, 0, steps + g, 0, 0)),
            pl.BlockSpec((parts, span, 1, 8, wide), lambda g: (0, 0, 2 * blocks, 0, 0)),
        ]
    return pl.pallas_call(
        partial(transform_kernel, parts=parts, count=count, span=span, group=group),
        grid=(steps,),
        in_specs=specs,
        out_specs=pl.BlockSpec((parts, 2 * count + 1, 8 * group, wide), lambda g: (0, 0, g, 0)),
        out_shape=jax.ShapeDtypeStruct((parts, 2 * count + 1, rows, wide), jnp.float32),
        scratch_shapes=[pltpu.VMEM((RADIX, RADIX, 8, wide), jnp.float32)] * 2,
        name="transform",
    )(*ins)


def exchange(values):
    moved = lax.all_to_all(
        values.astype(jnp.float16), "af", split_axis=0, concat_axis=0, tiled=True
    )
    return moved.astype(jnp.float32)


def everywhere(values, sizes):
    total = sizes[0] * sizes[1]
    step = 1
    while step < total:
        pairs = [(i, i ^ step) for i in range(total)]
        values = values + lax.ppermute(values, ("af", "sa"), pairs)
        step *= 2
    return values


def on_device(data_r, data_i, wave_r, wave_i, primaries_r, primaries_i, *, sizes):
    parts, ring = sizes
    count, rows, n = data_r.shape
    total_f = count * parts
    span = count // CHUNKS
    wholes = []
    for c in range(CHUNKS):
        cut = slice(c * span, (c + 1) * span)
        mine = jnp.stack([data_r[cut], data_i[cut]])
        if rows % 16 == 0:
            wholes.append(lax.all_gather(mine, "sa"))
        else:
            wholes.append(lax.all_gather(mine, "sa", axis=2, tiled=True))
    current = (primaries_r, primaries_i)
    sums = []
    for _ in range(ITERS):
        pieces, partials = [], []
        for c in range(CHUNKS):
            z, s = product(c, wave_r, wave_i, current, data_r, data_i, wholes[c], parts)
            pieces.append(exchange(z))
            partials.append(s)
        sums.append(sum(jnp.sum(s) for s in partials))
        current = exchange(transform(pieces, rows))
    misfit = everywhere(jnp.stack(sums), sizes) / (total_f * n * n)
    scale = jnp.exp2(current[:, 2 * count] - TOP)[:, None]

    def whole_rows(part):
        return (part * scale).transpose(1, 2, 0, 3).reshape(count, rows, n)

    return whole_rows(current[:, :count]), whole_rows(current[:, count : 2 * count]), misfit


def solution(mesh):
    spec = P("af", "sa", None)
    sizes = (mesh.shape["af"], mesh.shape["sa"])
    return jax.shard_map(
        partial(on_device, sizes=sizes),
        mesh=mesh,
        in_specs=(spec, spec, P("af"), P("af"), spec, spec),
        out_specs=(spec, spec, P()),
        check_vma=False,
    )
```

```python
import math
from functools import partial

import jax
import jax.numpy as jnp
from jax import lax
from jax.experimental import pallas as pl
from jax.experimental.pallas import tpu as pltpu
from jax.sharding import PartitionSpec as P

ITERS = 2
STEP_LENGTH = 0.02
THRESHOLD = 0.25
CHUNKS = 4
MOST_RING = 8
GROUPS = 2
TOP = 15.0
TINY = 1e-30
RADIX = 8
HALF = math.sqrt(0.5)


def add(a, b):
    return (a[0] + b[0], a[1] + b[1])


def sub(a, b):
    return (a[0] - b[0], a[1] - b[1])


def turn(a, sign):
    return (-a[1], a[0]) if sign > 0 else (a[1], -a[0])


def dft4(x, sign):
    a, b = add(x[0], x[2]), sub(x[0], x[2])
    c, d = add(x[1], x[3]), turn(sub(x[1], x[3]), sign)
    return [add(a, c), add(b, d), sub(a, c), sub(b, d)]


def dft8(x, sign):
    even, odd = dft4(x[0::2], sign), dft4(x[1::2], sign)
    r, i = odd[1]
    w1 = (HALF * (r - i), HALF * (i + r)) if sign > 0 else (HALF * (r + i), HALF * (i - r))
    w2 = turn(odd[2], sign)
    r, i = odd[3]
    w3 = (HALF * (-r - i), HALF * (r - i)) if sign > 0 else (HALF * (i - r), HALF * (-i - r))
    odd = [odd[0], w1, w2, w3]
    return [add(even[k], odd[k]) for k in range(4)] + [sub(even[k], odd[k]) for k in range(4)]


def twiddle(a, k, total, sign):
    if k % total == 0:
        return a
    c = math.cos(2.0 * math.pi * k / total)
    s = sign * math.sin(2.0 * math.pi * k / total)
    return (a[0] * c - a[1] * s, a[0] * s + a[1] * c)


def exponent(largest):
    return jnp.ceil(jnp.log2(jnp.maximum(largest, TINY))) + 1.0


def shrink(values):
    return values - jnp.clip(values, -THRESHOLD, THRESHOLD)


def gathered(slots, slot_ranks, p_scr):
    rows = slots[0].shape[2]
    for d, ref in enumerate(slots):
        at = pl.ds(pl.multiple_of(slot_ranks[d] * rows, rows), rows)
        p_scr[0, at] = ref[0, 0]
        p_scr[1, at] = ref[1, 0]
    return p_scr[0], p_scr[1]


def product_kernel(*refs, packed, parts, base, stacked_rows, slots):
    if slots:
        p_scr = refs[-1]
        z_out, sum_out = refs[-3:-1]
        ranks, whole = refs[-4 - slots], refs[-3 - slots : -3]
        refs = refs[: -4 - slots]
    else:
        z_out, sum_out = refs[-2:]
        whole = refs[-3]
        refs = refs[:-3]
    if packed:
        wr, wi, g_real, g_imag, g_exp, own_r, own_i = refs
        scale = jnp.exp2(g_exp[:, 0] - TOP)
        now_r = jnp.concatenate([g_real[d, 0] * scale[d] for d in range(parts)], axis=1)
        now_i = jnp.concatenate([g_imag[d, 0] * scale[d] for d in range(parts)], axis=1)
    else:
        wr, wi, g_real, g_imag, own_r, own_i = refs
        now_r = g_real[0]
        now_i = g_imag[0]
    f = base + pl.program_id(0)
    qr, qi = wr[f], wi[f]
    rows, n = now_r.shape
    if slots:
        p_r, p_i = gathered(whole, ranks, p_scr)
    elif stacked_rows:
        p_r = whole[:, 0, 0].reshape(n, n)
        p_i = whole[:, 1, 0].reshape(n, n)
    else:
        p_r = whole[0, 0]
        p_i = whole[1, 0]
    left = jnp.concatenate([now_r, now_i], axis=0).astype(jnp.bfloat16)
    with_r = jnp.dot(left, p_r, preferred_element_type=jnp.float32)
    with_i = jnp.dot(left, p_i, preferred_element_type=jnp.float32)
    e_r = own_r[0].astype(jnp.float32) + (with_r[:rows] - with_i[rows:]) - (qr * now_r - qi * now_i)
    e_i = own_i[0].astype(jnp.float32) + (with_i[:rows] + with_r[rows:]) - (qr * now_i + qi * now_r)
    wide = n // parts
    squares = (e_r * e_r + e_i * e_i).reshape(rows // 8, 8, n).sum(axis=0)
    total = squares[:, :wide]
    for d in range(1, parts):
        total = total + squares[:, d * wide : (d + 1) * wide]
    sum_out[0] = total
    eb = jnp.concatenate([e_r, e_i], axis=0).astype(jnp.bfloat16)
    dims = (((1,), (1,)), ((), ()))
    back_r = lax.dot_general(eb, p_r, dims, preferred_element_type=jnp.float32)
    back_i = lax.dot_general(eb, p_i, dims, preferred_element_type=jnp.float32)
    h_r = qr * e_r + qi * e_i - (back_r[:rows] + back_i[rows:])
    h_i = qr * e_i - qi * e_r - (back_r[rows:] - back_i[:rows])
    z_r = now_r + STEP_LENGTH * h_r
    z_i = now_i + STEP_LENGTH * h_i
    blocks = rows // 8
    cut_r = [z_r[:, d * wide : (d + 1) * wide].reshape(blocks, 8, wide) for d in range(parts)]
    cut_i = [z_i[:, d * wide : (d + 1) * wide].reshape(blocks, 8, wide) for d in range(parts)]
    largest = jnp.maximum(jnp.abs(cut_r[0]), jnp.abs(cut_i[0]))
    for d in range(1, parts):
        largest = jnp.maximum(largest, jnp.maximum(jnp.abs(cut_r[d]), jnp.abs(cut_i[d])))
    power = exponent(largest.max(axis=0))
    factor = jnp.exp2(TOP - power)
    for d in range(parts):
        z_out[d, 0, :blocks] = cut_r[d] * factor[None]
        z_out[d, 0, blocks : 2 * blocks] = cut_i[d] * factor[None]
        z_out[d, 0, 2 * blocks] = power


def product(chunk, wave_r, wave_i, current, data_r, data_i, whole, parts, ranks):
    packed = not isinstance(current, tuple)
    count, rows, n = data_r.shape
    span = count // CHUNKS
    base = chunk * span
    wide = n // parts
    blocks = rows // 8
    slots = len(whole) if isinstance(whole, list) else 0
    stacked_rows = not slots and whole.ndim == 5
    smem = pl.BlockSpec(memory_space=pltpu.SMEM)
    own = pl.BlockSpec((1, rows, n), lambda f: (base + f, 0, 0))
    if packed:
        ins = [current, current, current]
        held = current.shape[1] // 2
        first = base % held
        cur = [
            pl.BlockSpec((parts, 1, rows, wide), lambda f: (0, first + f, 0, 0)),
            pl.BlockSpec((parts, 1, rows, wide), lambda f: (0, held + first + f, 0, 0)),
            pl.BlockSpec((parts, 1, rows, wide), lambda f: (0, 2 * held, 0, 0)),
        ]
    else:
        ins = list(current)
        cur = [own, own]
    scratch = []
    if slots:
        far = [smem] + [pl.BlockSpec((2, 1, rows, n), lambda f: (0, f, 0, 0))] * slots
        tail = [ranks] + whole
        scratch = [pltpu.VMEM((2, n, n), jnp.bfloat16)]
    elif stacked_rows:
        far = [pl.BlockSpec((whole.shape[0], 2, 1, rows, n), lambda f: (0, 0, f, 0, 0))]
        tail = [whole]
    else:
        far = [pl.BlockSpec((2, 1, n, n), lambda f: (0, f, 0, 0))]
        tail = [whole]
    kernel = partial(
        product_kernel,
        packed=packed,
        base=base,
        parts=parts,
        stacked_rows=stacked_rows,
        slots=slots,
    )
    return pl.pallas_call(
        kernel,
        grid=(span,),
        in_specs=[smem, smem] + cur + [own, own] + far,
        scratch_shapes=scratch,
        out_specs=[
            pl.BlockSpec((parts, 1, 2 * blocks + 1, 8, wide), lambda f: (0, f, 0, 0, 0)),
            pl.BlockSpec((1, 8, wide), lambda f: (f, 0, 0)),
        ],
        out_shape=[
            jax.ShapeDtypeStruct((parts, span, 2 * blocks + 1, 8, wide), jnp.float32),
            jax.ShapeDtypeStruct((span, 8, wide), jnp.float32),
        ],
        cost_estimate=pl.CostEstimate(
            flops=span * 16 * rows * n * n, bytes_accessed=span * 6 * n * n, transcendentals=0
        ),
        name=f"product_{chunk}_{int(packed)}",
    )(wave_r, wave_i, *ins, data_r, data_i, *tail)


def transform_kernel(*refs, parts, count, span, group, held):
    ins, outs = refs[: 3 * CHUNKS], refs[3 * CHUNKS : -2]
    buf_r, buf_i = refs[-2:]
    total = parts * count
    norm = 1.0 / math.sqrt(total)

    def one(b, carry):
        def load(f):
            src, rest = divmod(f, count)
            chunk, j = divmod(rest, span)
            re, im, ex = ins[3 * chunk : 3 * chunk + 3]
            scale = jnp.exp2(ex[src, j, 0] - TOP) * norm
            return (re[src, j, b] * scale, im[src, j, b] * scale)

        for f0 in range(RADIX):
            got = dft8([load(RADIX * f1 + f0) for f1 in range(RADIX)], 1)
            for t1 in range(RADIX):
                v = twiddle(got[t1], f0 * t1, total, 1)
                buf_r[f0, t1], buf_i[f0, t1] = v
        largest = None
        for t1 in range(RADIX):
            z = dft8([(buf_r[f0, t1], buf_i[f0, t1]) for f0 in range(RADIX)], 1)
            x = [(shrink(r), shrink(i)) for r, i in z]
            for r, i in x:
                m = jnp.maximum(jnp.abs(r), jnp.abs(i))
                largest = m if largest is None else jnp.maximum(largest, m)
            got = dft8(x, -1)
            for f0 in range(RADIX):
                v = twiddle(got[f0], f0 * t1, total, -1)
                buf_r[f0, t1], buf_i[f0, t1] = v
        power = exponent(largest * (1.5 * math.sqrt(total)))
        factor = jnp.exp2(TOP - power) * norm
        at = pl.ds(pl.multiple_of(b * 8, 8), 8)
        for f0 in range(RADIX):
            got = dft8([(buf_r[f0, t1], buf_i[f0, t1]) for t1 in range(RADIX)], -1)
            for f1 in range(RADIX):
                dst, rest = divmod(RADIX * f1 + f0, count)
                which, j = divmod(rest, held)
                outs[which][dst, j, at] = got[f1][0] * factor
                outs[which][dst, held + j, at] = got[f1][1] * factor
        for dst in range(parts):
            for out in outs:
                out[dst, 2 * held, at] = power
        return carry

    lax.fori_loop(0, group, one, 0)


def transform(pieces, rows, groups):
    parts, span, _, _, wide = pieces[0].shape
    count = span * CHUNKS
    blocks = rows // 8
    group = 2 if blocks % 2 == 0 else 1
    steps = blocks // group
    held = count // groups
    specs, ins = [], []
    for piece in pieces:
        ins += [piece] * 3
        specs += [
            pl.BlockSpec((parts, span, group, 8, wide), lambda g: (0, 0, g, 0, 0)),
            pl.BlockSpec((parts, span, group, 8, wide), lambda g: (0, 0, steps + g, 0, 0)),
            pl.BlockSpec((parts, span, 1, 8, wide), lambda g: (0, 0, 2 * blocks, 0, 0)),
        ]
    return pl.pallas_call(
        partial(
            transform_kernel, parts=parts, count=count, span=span, group=group, held=held
        ),
        grid=(steps,),
        in_specs=specs,
        out_specs=[pl.BlockSpec((parts, 2 * held + 1, 8 * group, wide), lambda g: (0, 0, g, 0))]
        * groups,
        out_shape=[jax.ShapeDtypeStruct((parts, 2 * held + 1, rows, wide), jnp.float32)] * groups,
        scratch_shapes=[pltpu.VMEM((RADIX, RADIX, 8, wide), jnp.float32)] * 2,
        name="transform",
    )(*ins)


def after(value, *others):
    return lax.optimization_barrier((value, *others))[0]


def send(values):
    return lax.all_to_all(
        values.astype(jnp.float16), "af", split_axis=0, concat_axis=0, tiled=True
    )


def exchange(values):
    return send(values).astype(jnp.float32)


def add_partner(values, step, total):
    pairs = [(i, i ^ step) for i in range(total)]
    return values + lax.ppermute(values, ("af", "sa"), pairs)


def ring_pairs(c, ring):
    way = 1 if c % 2 == 0 else -1
    return [(i, (i + 2 * way) % ring) for i in range(ring)]


def slot_ranks(c, ring):
    chips = ring // 2
    place = lax.axis_index("sa")
    way = 1 if c % 2 == 0 else -1
    steps = jnp.arange(chips, dtype=jnp.int32) * (2 * way)
    same = (place - steps + 2 * ring) % ring
    return jnp.concatenate([same, same ^ 1]).astype(jnp.int32)


def on_device(data_r, data_i, wave_r, wave_i, primaries_r, primaries_i, *, sizes):
    parts, ring = sizes
    total = parts * ring
    count, rows, n = data_r.shape
    span = count // CHUNKS
    chunks = []
    for c in range(CHUNKS):
        cut = slice(c * span, (c + 1) * span)
        chunks.append(jnp.stack([data_r[cut], data_i[cut]]))
    ring_form = 4 < ring <= MOST_RING and rows % 16 == 0
    ranks = [slot_ranks(c, ring) if ring_form else None for c in range(CHUNKS)]
    wholes = [None] * CHUNKS

    def step(c, current):
        return product(c, wave_r, wave_i, current, data_r, data_i, wholes[c], parts, ranks[c])

    start = (primaries_r, primaries_i)
    firsts = [None] * CHUNKS
    if ring_form:
        swap = [(i, i ^ 1) for i in range(ring)]
        chips = ring // 2
        before = None
        for c in range(CHUNKS):
            slots = [chunks[c]]
            if c:
                slots[0] = after(slots[0], before[-2])
            for d in range(1, chips):
                source = slots[-1]
                if d == chips - 1 and c:
                    source = after(source, firsts[c - 1][0])
                slots.append(lax.ppermute(source, "sa", ring_pairs(c, ring)))
                if d == 1 and c:
                    firsts[c - 1] = step(c - 1, start)
            before = slots
            wholes[c] = slots + [lax.ppermute(slot, "sa", swap) for slot in slots]
        firsts[-1] = step(CHUNKS - 1, start)
    else:
        for c in range(CHUNKS):
            if rows % 16 == 0:
                wholes[c] = lax.all_gather(chunks[c], "sa")
            else:
                wholes[c] = lax.all_gather(chunks[c], "sa", axis=2, tiled=True)
            firsts[c] = step(c, start)
    sums = [sum(jnp.sum(s) for _, s in firsts)]
    pieces = [exchange(z) for z, _ in firsts]
    shares = CHUNKS // GROUPS
    for iteration in range(1, ITERS):
        groups = transform(pieces, rows, GROUPS)
        pieces, partials = [], []
        for g, group in enumerate(groups):
            if g > 1:
                group = after(group, latest)
            current = exchange(group)
            for c in range(g * shares, (g + 1) * shares):
                latest, s = step(c, current)
                pieces.append(exchange(latest))
                partials.append(s)
        sums.append(sum(jnp.sum(s) for s in partials))
    values = jnp.stack(sums)
    hop = 1
    while hop < total:
        values = add_partner(values, hop, total)
        if hop == 2:
            pieces[-1] = after(pieces[-1], values)
        hop *= 2
    misfit = values / (count * parts * n * n)
    last = exchange(transform(pieces, rows, 1)[0])
    scale = jnp.exp2(last[:, 2 * count] - TOP)[:, None]

    def whole_rows(part):
        return (part * scale).transpose(1, 2, 0, 3).reshape(count, rows, n)

    return whole_rows(last[:, :count]), whole_rows(last[:, count : 2 * count]), misfit


def solution(mesh):
    spec = P("af", "sa", None)
    sizes = (mesh.shape["af"], mesh.shape["sa"])
    return jax.shard_map(
        partial(on_device, sizes=sizes),
        mesh=mesh,
        in_specs=(spec, spec, P("af"), P("af"), spec, spec),
        out_specs=(spec, spec, P()),
        check_vma=False,
    )
```
